32 devices in a mesh: expert: 8 (over y, x, core), replica: 4 (over z).
Axes of the slice: x: 2, y: 2, z: 4, core: 2. Of those that a mesh axis runs over, the one named last changes fastest.
Arguments:
- tokens_in: bfloat16 [8192, 2048], P(('expert', 'replica')), may hold values from -6 to 6
- cotangents: bfloat16 [8192, 8192], P(('expert', 'replica')), may hold values from -0.1796875 to 0.1796875
- left_root: bfloat16 [8, 2048, 2048], P('expert'), may hold values from -2 to 6, as said below
- right_root: bfloat16 [8, 8, 1024, 1024], P('expert', 'replica'), may hold values from -2 to 6, as said below
Outputs:
- update: bfloat16 [8, 2048, 8192], P('expert', None, 'replica')
The draws below stay inside these ranges and needn't reach their ends.
Inputs may be any that keep to these rules, and one draw needn't show every extreme that they name: `left_root`: each matrix is symmetric. `right_root`: each block is symmetric.
All inputs are finite; a program needn't handle non-finite values.
Results may differ from the reference program's by a relative error of at most 0.0058.
Values may be sent and summed in bfloat16 or wider, within the bound.
A program may use at most 192 MiB of HBM per device.

```python
import math
import jax
import jax.numpy as jnp
from jax import lax

D = 2048
FF = 8192
BLOCK = 1024
EXPERTS = 8
SLOTS = 32
TOKENS = 8192
BLOCKS = 8


def factor_draw(key, leading, order):
    diag_key, noise_key = jax.random.split(key)
    diagonal = jnp.exp(jax.random.uniform(diag_key, leading + (order,), jnp.float32, 0.0, math.log(3.0)))
    random_part = jnp.clip(jax.random.normal(noise_key, leading + (order, order), jnp.float32), -4.0, 4.0)
    random_part = random_part * (0.8 / math.sqrt(order))
    symmetric = 0.5 * (random_part + jnp.swapaxes(random_part, -1, -2))
    identity = jnp.eye(order, dtype=jnp.float32)
    return (symmetric + identity * diagonal[..., None]).astype(jnp.bfloat16)


def draw_left_root(key, part):
    return factor_draw(jax.random.fold_in(key, 11), (EXPERTS,), D)


def draw_right_root(key, part):
    return factor_draw(jax.random.fold_in(key, 12), (EXPERTS, BLOCKS), BLOCK)


def block_scale(rng, dims, cuts, smallest, top_value):
    loudness = 1.0
    for position, shards_of in cuts:
        steps = jax.random.uniform(jax.random.fold_in(jax.random.fold_in(rng, 6), position), (shards_of,), jnp.float32, smallest / len(cuts), top_value / len(cuts))
        loudness = loudness * jnp.repeat(jnp.exp(steps), dims[position] // shards_of).reshape((-1,) + (1,) * (len(dims) - 1 - position))
    return loudness


def centred(stream_key, dims, spread, most, shards=(), kind=jnp.bfloat16):
    values = jax.random.normal(stream_key, dims, jnp.float32) * spread
    if len(shards) > 0:
        values = block_scale(stream_key, dims, shards, -0.22, 0.18) * values
    return jnp.clip(values, min=-most, max=most).astype(kind)


def setup_inputs(seed: int = 0) -> dict:
    streams_of = jax.random.split(jax.random.key(seed), 5)
    return {
        "tokens_in": centred(streams_of[0], (TOKENS, D), 1.0, 6.0, ((0, 32),)),
        "cotangents": centred(streams_of[1], (TOKENS, FF), 0.03, 0.1796875, ((0, 32),)),
        "left_root": draw_left_root(jax.random.fold_in(streams_of[4], 71), 0),
        "right_root": draw_right_root(jax.random.fold_in(streams_of[4], 71), 0),
    }


def per_expert(inputs):
    expert_tokens, expert_cotangents, left_factor, right_factor = inputs
    gradient = jnp.dot(expert_tokens.T, expert_cotangents, preferred_element_type=jnp.float32).astype(jnp.bfloat16)
    blocks = gradient.reshape(D, BLOCKS, BLOCK).astype(jnp.float32)
    applied = jnp.einsum("dbk,bkj->dbj", blocks, right_factor.astype(jnp.float32))
    applied = applied.astype(jnp.bfloat16).reshape(D, FF)
    return jnp.dot(left_factor, applied, preferred_element_type=jnp.float32).astype(jnp.bfloat16)


def reference(tokens_in, cotangents, left_root, right_root):
    token_groups = jnp.moveaxis(tokens_in.reshape(-1, EXPERTS, SLOTS, D), 1, 0).reshape(EXPERTS, -1, D)
    cotangent_groups = jnp.moveaxis(cotangents.reshape(-1, EXPERTS, SLOTS, FF), 1, 0).reshape(EXPERTS, -1, FF)
    return lax.map(per_expert, (token_groups, cotangent_groups, left_root, right_root))
```

```python
import functools
import jax
import jax.numpy as jnp
from jax import lax
from jax.experimental import pallas as pl
from jax.experimental.pallas import tpu as pltpu
from jax.sharding import PartitionSpec as P

LEAD, C1, C2 = 1, 0, 0
XM, PN, FM, FN = 1024, 256, 512, 256


def tile_of(size, most):
    return most if size % most == 0 else size


def route_kernel(
    ne, nr, tok_ref, cot_ref, left_ref, right_ref, part_ref, x_late, y_late,
    tok, cot, left, right, x, y,
    plane_send, up_send, down_send, cot_send, tok_recv, cot_recv, local,
):
    e = lax.axis_index("expert")
    r = lax.axis_index("replica")
    rows = tok_ref.shape[0] // ne
    group = rows * ne
    half = group // 2
    width = tok.shape[1]
    cols = cot.shape[1]
    blocks, order = right_ref.shape[0], right_ref.shape[1]

    nc = 2 if ne % 2 == 0 else 1
    nx = 2 if ne % (2 * nc) == 0 else 1
    ny = ne // (nc * nx)
    core = e % nc
    self_k = core * (nx * ny - 1)

    def target_of(k):
        dx, dy, dc = k + core, k // nx + core, k // (nx * ny)
        return ((e // (nc * nx) + dy) % ny * nx + (e // nc + dx) % nx) * nc + (core + dc) % nc

    def at_rows(start, size):
        return pl.ds(pl.multiple_of(start, rows), size)

    def tok_at(origin, k):
        return at_rows((origin * ne + k) * rows, rows)

    def place(tr, origin):
        return jnp.where(tr >= nr // 2, origin + nr - tr, tr + nr - origin) % nr

    def cot_at(tr, origin, k):
        i = place(tr, origin)
        second = k // (ne // 2)
        split = (nr - 2) * group + second * group + (i - (nr - 2)) * half + (k - second * (ne // 2)) * rows
        return at_rows(jnp.where(i < nr - 2, i * group + k * rows, split), rows)

    def own_rows(target):
        return at_rows(target * rows, rows)

    def own_cols(target):
        return pl.ds(pl.multiple_of(target * cols, cols), cols)

    def plane_copy(k):
        target = target_of(k)
        return pltpu.make_async_remote_copy(
            tok_ref.at[own_rows(target)], tok.at[tok_at(r, k)],
            plane_send, tok_recv.at[r * ne + k],
            device_id={"expert": target, "replica": r},
        )

    def relay(origin, k, up, src):
        return pltpu.make_async_remote_copy(
            src, tok.at[tok_at(origin, k)],
            up_send if up else down_send, tok_recv.at[origin * ne + k],
            device_id={"expert": e, "replica": r + 1 if up else r - 1},
        )

    def forward(origin, k, up, src):
        ahead = (r + 1 < nr) if up else (r > 0)

        @pl.when(ahead)
        def _():
            relay(origin, k, up, src).start()

    def tok_wait(origin, k):
        pltpu.make_async_remote_copy(
            tok.at[tok_at(origin, k)], tok.at[tok_at(origin, k)],
            up_send, tok_recv.at[origin * ne + k],
            device_id={"expert": e, "replica": (r + 1) % nr},
        ).wait_recv()

    def cot_copy(k, tr):
        te = target_of(k)
        return pltpu.make_async_remote_copy(
            cot_ref.at[own_rows(te), own_cols(tr)], cot.at[cot_at(tr, r, k)],
            cot_send, cot_recv.at[r * 2 + k // (ne // 2)],
            device_id={"expert": te, "replica": tr},
        )

    def cot_wait(origin, second):
        whole = cot.at[pl.ds(0, half)]
        pltpu.make_async_remote_copy(
            whole, whole, cot_send, cot_recv.at[origin * 2 + second],
            device_id={"expert": e, "replica": (r + 1) % nr},
        ).wait_recv()

    barrier = pltpu.get_barrier_semaphore()

    @pl.loop(1, ne * nr)
    def _(k):
        pl.semaphore_signal(
            barrier, inc=1,
            device_id={"expert": (e + k % ne) % ne, "replica": (r + k // ne) % nr},
        )

    own_tok = tok_ref.at[own_rows(e)]
    pltpu.make_async_copy(own_tok, tok.at[tok_at(r, self_k)], tok_recv.at[r * ne + self_k]).start()
    pltpu.make_async_copy(
        cot_ref.at[own_rows(e), own_cols(r)], cot.at[cot_at(r, r, self_k)], cot_recv.at[r * 2]
    ).start()
    load_left = pltpu.make_async_copy(left_ref, left, local.at[0])
    load_right = pltpu.make_async_copy(right_ref, right, local.at[1])
    load_left.start()
    load_right.start()
    with jax.named_scope("bar"):
        pl.semaphore_wait(barrier, ne * nr - 1)

    @pl.loop(0, ne)
    def _(k):
        @pl.when(k != self_k)
        def _():
            plane_copy(k).start()

    def send_targets(first, end):
        @pl.loop(first, end)
        def _(k):
            def send(distances):
                for distance in distances:
                    for tr in (r + distance, r - distance):
                        @pl.when((tr >= 0) & (tr < nr))
                        def _():
                            cot_copy(k, tr).start()

            @pl.when(core == 0)
            def _():
                send(range(nr - 1, 0, -1))

            @pl.when(core != 0)
            def _():
                send(range(1, nr))

    send_targets(0, LEAD)
    forward(r, self_k, True, own_tok)
    forward(r, self_k, False, own_tok)

    with jax.named_scope("plane"):
        @pl.loop(0, ne)
        def _(k):
            @pl.when(k != self_k)
            def _():
                tok_wait(r, k)
                forward(r, k, True, tok.at[tok_at(r, k)])
                forward(r, k, False, tok.at[tok_at(r, k)])

    def relay_step(distance, k):
        for origin, up in ((r - distance, True), (r + distance, False)):
            @pl.when((origin >= 0) & (origin < nr))
            def _():
                tok_wait(origin, k)
                forward(origin, k, up, tok.at[tok_at(origin, k)])

    sent = LEAD
    for distance in range(1, nr - 1):
        more = (C1, C2)[distance - 1] if distance < 3 else 0
        with jax.named_scope("relay%d" % distance):
            @pl.loop(0, ne)
            def _(k):
                relay_step(distance, k)

                if distance == 1:
                    @pl.when(k != self_k)
                    def _():
                        cot_copy(k, r).start()

                if more:
                    @pl.when(k < more)
                    def _():
                        send_targets(sent + k, sent + k + 1)
        sent += more

    send_targets(sent, ne)

    planes = [jnp.where(r >= nr // 2, r + i, r + nr - i) % nr for i in range(nr)]

    with jax.named_scope("relay%d" % (nr - 1)):
        @pl.loop(0, ne)
        def _(k):
            relay_step(nr - 1, k)

    load_left.wait()
    tok_wait(r, self_k)
    step = tile_of(width, XM)
    for i, g in enumerate(planes):
        with jax.named_scope("x%d" % i):
            @pl.loop(0, width // step)
            def _(j):
                part = pl.ds(pl.multiple_of(j * step, step), step)
                columns = pl.ds(pl.multiple_of(g * group, group), group)
                tile = lax.dot_general(
                    left[part, :], tok[columns, :], (((1,), (1,)), ((), ())),
                    preferred_element_type=jnp.float32,
                ).astype(x.dtype)
                if i < nr - 2:
                    x[part, i * group:(i + 1) * group] = tile
                else:
                    at = (i - (nr - 2)) * half
                    x[part, (nr - 2) * group + at:(nr - 2) * group + at + half] = tile[:, :half]
                    x_late[part, at:at + half] = tile[:, half:]

    load_right.wait()

    def make_y(i, out):
        for b in range(blocks):
            inside = slice(b * order, (b + 1) * order)
            out[:, inside] = jnp.dot(
                cot[i * group:(i + 1) * group, inside], right[b], preferred_element_type=jnp.float32
            ).astype(y.dtype)

    for i in range(nr - 2):
        with jax.named_scope("yw%d" % i):
            cot_wait(planes[i], 0)
            cot_wait(planes[i], 1)
        make_y(i, y.at[i * group:(i + 1) * group])

    with jax.named_scope("ywhalf"):
        cot_wait(planes[nr - 2], 0)
        cot_wait(planes[nr - 1], 0)
    make_y(nr - 2, y.at[(nr - 2) * group:(nr - 1) * group])

    with jax.named_scope("P"):
        step = tile_of(cols, PN)

        @pl.loop(0, cols // step)
        def _(j):
            part = pl.ds(pl.multiple_of(j * step, step), step)
            part_ref[:, part] = jnp.dot(x[...], y[:, part], preferred_element_type=jnp.float32)

    def send_wait(sem, data):
        pltpu.make_async_remote_copy(
            data, data, sem, tok_recv.at[0], device_id={"expert": e, "replica": (r + 1) % nr}
        ).wait_send()

    with jax.named_scope("sends"):
        send_wait(plane_send, tok.at[pl.ds(0, group - rows)])
        send_wait(cot_send, cot.at[pl.ds(0, group * nr - rows)])
        for q in range(1, nr):
            @pl.when(r + 1 == q)
            def _():
                send_wait(up_send, tok.at[pl.ds(0, q * group)])

            @pl.when(nr - r == q)
            def _():
                send_wait(down_send, tok.at[pl.ds(0, q * group)])

    with jax.named_scope("ywlate"):
        cot_wait(planes[nr - 2], 1)
        cot_wait(planes[nr - 1], 1)
    make_y(nr - 1, y_late)


def finish_kernel(part_ref, x_ref, y_ref, out_ref):
    rows, cols = out_ref.shape
    at = pl.ds(pl.multiple_of(pl.program_id(0) * rows, rows), rows)
    step = tile_of(cols, FN)
    for j in range(cols // step):
        part = slice(j * step, (j + 1) * step)
        out_ref[:, part] = (
            part_ref[at, part]
            + jnp.dot(x_ref[at, :], y_ref[:, part], preferred_element_type=jnp.float32)
        ).astype(out_ref.dtype)


def body(tokens_in, cotangents, left_root, right_root):
    ne, nr = lax.axis_size("expert"), lax.axis_size("replica")
    assert left_root.shape[0] == 1
    width = tokens_in.shape[1]
    columns = cotangents.shape[1] // nr
    total = tokens_in.shape[0] * nr
    group = tokens_in.shape[0]
    blocks, order = right_root.shape[1], right_root.shape[2]
    anywhere = pl.BlockSpec(memory_space=pl.ANY)
    vmem = pl.BlockSpec(memory_space=pltpu.VMEM)
    dtype = jnp.bfloat16
    dma = pltpu.SemaphoreType.DMA
    part, x_late, y_late = pl.pallas_call(
        functools.partial(route_kernel, ne, nr),
        out_shape=[
            pltpu.VMEM((width, columns), jnp.float32),
            pltpu.VMEM((width, group), dtype),
            pltpu.VMEM((group, columns), dtype),
        ],
        in_specs=[anywhere] * 4,
        out_specs=[vmem] * 3,
        scratch_shapes=[
            pltpu.VMEM((total, width), dtype),
            pltpu.VMEM((total, columns), dtype),
            pltpu.VMEM((width, width), dtype),
            pltpu.VMEM((blocks, order, order), dtype),
            pltpu.VMEM((width, total - group), dtype),
            pltpu.VMEM((total - group, columns), dtype),
            dma, dma, dma, dma, dma((ne * nr,)), dma((2 * nr,)), dma((2,)),
        ],
        compiler_params=pltpu.CompilerParams(
            collective_id=0, has_side_effects=True, vmem_limit_bytes=38 * 1024 * 1024
        ),
    )(tokens_in, cotangents, left_root[0], right_root[0])
    step = tile_of(width, FM)
    out = pl.pallas_call(
        finish_kernel,
        out_shape=jax.ShapeDtypeStruct((width, columns), dtype),
        grid=(width // step,),
        in_specs=[vmem] * 3,
        out_specs=pl.BlockSpec((step, columns), lambda i: (i, 0)),
        compiler_params=pltpu.CompilerParams(vmem_limit_bytes=12 * 1024 * 1024),
    )(part, x_late, y_late)
    return out[None]


def solution(mesh):
    in_specs = (
        P(("expert", "replica"), None),
        P(("expert", "replica"), None),
        P("expert", None, None),
        P("expert", "replica", None, None),
    )
    out_specs = P("expert", None, "replica")
    return jax.shard_map(body, mesh=mesh, in_specs=in_specs, out_specs=out_specs, check_vma=False)
```

```python
import functools
import jax
import jax.numpy as jnp
from jax import lax
from jax.experimental import pallas as pl
from jax.experimental.pallas import tpu as pltpu
from jax.sharding import PartitionSpec as P

LEAD, C1, C2, AHEAD = 1, 0, 1, 1
XM, PN, FM = 1024, 256, 256


def tile_of(size, most):
    return most if size % most == 0 else size


def route_kernel(
    ne, nr, tok_ref, cot_ref, left_ref, right_ref, x_late, cot, right, part_ref,
    tok, left, x, y, low, high,
    plane_send, up_send, down_send, cot_send, tok_recv, cot_recv, local,
):
    e = lax.axis_index("expert")
    r = lax.axis_index("replica")
    rows = tok_ref.shape[0] // ne
    group = rows * ne
    half = group // 2
    width = tok.shape[1]
    cols = cot.shape[1]
    blocks, order = right_ref.shape[0], right_ref.shape[1]

    nc = 2 if ne % 2 == 0 else 1
    nx = 2 if ne % (2 * nc) == 0 else 1
    ny = ne // (nc * nx)
    core = e % nc
    self_k = core * (nx * ny - 1)

    def target_of(k):
        dx, dy, dc = k + core, k // nx + core, k // (nx * ny)
        return ((e // (nc * nx) + dy) % ny * nx + (e // nc + dx) % nx) * nc + (core + dc) % nc

    def at_rows(start, size):
        return pl.ds(pl.multiple_of(start, rows), size)

    def tok_at(origin, k):
        return at_rows((origin * ne + k) * rows, rows)

    def place(tr, origin):
        return jnp.where(tr >= nr // 2, origin + nr - tr, tr + nr - origin) % nr

    def cot_at(tr, origin, k):
        i = place(tr, origin)
        second = k // (ne // 2)
        split = (nr - 2) * group + second * group + (i - (nr - 2)) * half + (k - second * (ne // 2)) * rows
        return at_rows(jnp.where(i < nr - 2, i * group + k * rows, split), rows)

    def own_rows(target):
        return at_rows(target * rows, rows)

    def own_cols(target):
        return pl.ds(pl.multiple_of(target * cols, cols), cols)

    def plane_copy(k):
        target = target_of(k)
        return pltpu.make_async_remote_copy(
            tok_ref.at[own_rows(target)], tok.at[tok_at(r, k)],
            plane_send, tok_recv.at[r * ne + k],
            device_id={"expert": target, "replica": r},
        )

    def relay(origin, k, up, src):
        return pltpu.make_async_remote_copy(
            src, tok.at[tok_at(origin, k)],
            up_send if up else down_send, tok_recv.at[origin * ne + k],
            device_id={"expert": e, "replica": r + 1 if up else r - 1},
        )

    def forward(origin, k, up, src):
        ahead = (r + 1 < nr) if up else (r > 0)

        @pl.when(ahead)
        def _():
            relay(origin, k, up, src).start()

    def tok_wait(origin, k):
        pltpu.make_async_remote_copy(
            tok.at[tok_at(origin, k)], tok.at[tok_at(origin, k)],
            up_send, tok_recv.at[origin * ne + k],
            device_id={"expert": e, "replica": (r + 1) % nr},
        ).wait_recv()

    def cot_copy(k, tr):
        te = target_of(k)
        return pltpu.make_async_remote_copy(
            cot_ref.at[own_rows(te), own_cols(tr)], cot.at[cot_at(tr, r, k)],
            cot_send, cot_recv.at[r * 2 + k // (ne // 2)],
            device_id={"expert": te, "replica": tr},
        )

    def cot_wait(origin, second):
        whole = cot.at[pl.ds(0, half)]
        pltpu.make_async_remote_copy(
            whole, whole, cot_send, cot_recv.at[origin * 2 + second],
            device_id={"expert": e, "replica": (r + 1) % nr},
        ).wait_recv()

    barrier = pltpu.get_barrier_semaphore()
    above, below = r + 1 < nr, r > 0

    @pl.loop(1, ne)
    def _(k):
        pl.semaphore_signal(barrier, inc=1, device_id={"expert": (e + k) % ne, "replica": r})

    def tell(up, sem):
        @pl.when(above if up else below)
        def _():
            pl.semaphore_signal(sem, inc=1, device_id={"expert": e, "replica": r + 1 if up else r - 1})

    tell(True, barrier)
    tell(False, barrier)

    own_tok = tok_ref.at[own_rows(e)]
    pltpu.make_async_copy(own_tok, tok.at[tok_at(r, self_k)], tok_recv.at[r * ne + self_k]).start()
    pltpu.make_async_copy(
        cot_ref.at[own_rows(e), own_cols(r)], cot.at[cot_at(r, r, self_k)], cot_recv.at[r * 2]
    ).start()
    load_left = pltpu.make_async_copy(left_ref, left, local.at[0])
    load_right = pltpu.make_async_copy(right_ref, right, local.at[1])
    load_left.start()
    load_right.start()
    with jax.named_scope("bar"):
        pl.semaphore_wait(barrier, ne - 1 + above.astype(jnp.int32) + below.astype(jnp.int32))
    tell(True, low.at[0])
    tell(False, high.at[0])

    @pl.loop(0, ne)
    def _(k):
        @pl.when(k != self_k)
        def _():
            plane_copy(k).start()

    def send_cots(k, distance):
        for tr in (r + distance, r - distance):
            @pl.when((tr >= 0) & (tr < nr))
            def _():
                cot_copy(k, tr).start()

    steps = ne + AHEAD * (nr - 2)

    def send_targets(first, end):
        @pl.loop(first, end)
        def _(step):
            def send(distances):
                for distance in distances:
                    k = step - AHEAD * (nr - 1 - distance)
                    ok = (k >= 0) & (k < ne)

                    @pl.when(ok & (k != self_k) if distance == 1 else ok)
                    def _():
                        send_cots(k, distance)

            @pl.when(core == 0)
            def _():
                send(range(nr - 1, 0, -1))

            @pl.when(core != 0)
            def _():
                send(range(1, nr))

    forward(r, self_k, True, own_tok)
    forward(r, self_k, False, own_tok)
    send_cots(self_k, 1)

    with jax.named_scope("ready"):
        for distance in range(1, nr):
            @pl.when(r >= distance)
            def _():
                pl.semaphore_wait(low.at[distance - 1], 1)
                if distance + 1 < nr:
                    tell(True, low.at[distance])

            @pl.when(r + distance < nr)
            def _():
                pl.semaphore_wait(high.at[distance - 1], 1)
                if distance + 1 < nr:
                    tell(False, high.at[distance])

    send_targets(0, LEAD)

    with jax.named_scope("plane"):
        @pl.loop(0, ne)
        def _(k):
            @pl.when(k != self_k)
            def _():
                tok_wait(r, k)
                forward(r, k, True, tok.at[tok_at(r, k)])
                forward(r, k, False, tok.at[tok_at(r, k)])

    def relay_step(distance, k):
        for origin, up in ((r - distance, True), (r + distance, False)):
            @pl.when((origin >= 0) & (origin < nr))
            def _():
                tok_wait(origin, k)
                forward(origin, k, up, tok.at[tok_at(origin, k)])

    sent = LEAD
    for distance in range(1, nr - 1):
        more = (C1, C2)[distance - 1] if distance < 3 else 0
        with jax.named_scope("relay%d" % distance):
            @pl.loop(0, ne)
            def _(k):
                relay_step(distance, k)

                if distance == 1:
                    @pl.when(k != self_k)
                    def _():
                        cot_copy(k, r).start()

                if more:
                    @pl.when(k < more)
                    def _():
                        send_targets(sent + k, sent + k + 1)
        sent += more

    send_targets(sent, steps)

    planes = [jnp.where(r >= nr // 2, r + i, r + nr - i) % nr for i in range(nr)]

    with jax.named_scope("relay%d" % (nr - 1)):
        @pl.loop(0, ne)
        def _(k):
            relay_step(nr - 1, k)

    load_left.wait()
    tok_wait(r, self_k)
    step = tile_of(width, XM)
    for i, g in enumerate(planes):
        with jax.named_scope("x%d" % i):
            @pl.loop(0, width // step)
            def _(j):
                part = pl.ds(pl.multiple_of(j * step, step), step)
                columns = pl.ds(pl.multiple_of(g * group, group), group)
                tile = lax.dot_general(
                    left[part, :], tok[columns, :], (((1,), (1,)), ((), ())),
                    preferred_element_type=jnp.float32,
                ).astype(x.dtype)
                if i < nr - 2:
                    x[part, i * group:(i + 1) * group] = tile
                else:
                    at = (i - (nr - 2)) * half
                    x[part, (nr - 2) * group + at:(nr - 2) * group + at + half] = tile[:, :half]
                    x_late[part, at:at + half] = tile[:, half:]

    load_right.wait()

    def make_y(i, out):
        for b in range(blocks):
            inside = slice(b * order, (b + 1) * order)
            out[:, inside] = jnp.dot(
                cot[i * group:(i + 1) * group, inside], right[b], preferred_element_type=jnp.float32
            ).astype(y.dtype)

    for i in range(nr - 2):
        with jax.named_scope("yw%d" % i):
            cot_wait(planes[i], 0)
            cot_wait(planes[i], 1)
        make_y(i, y.at[i * group:(i + 1) * group])

    with jax.named_scope("ywhalf"):
        cot_wait(planes[nr - 2], 0)
        cot_wait(planes[nr - 1], 0)
    make_y(nr - 2, y.at[(nr - 2) * group:(nr - 1) * group])

    with jax.named_scope("P"):
        step = tile_of(cols, PN)

        @pl.loop(0, cols // step)
        def _(j):
            part = pl.ds(pl.multiple_of(j * step, step), step)
            part_ref[:, part] = jnp.dot(x[...], y[:, part], preferred_element_type=jnp.float32)

    def send_wait(sem, data):
        pltpu.make_async_remote_copy(
            data, data, sem, tok_recv.at[0], device_id={"expert": e, "replica": (r + 1) % nr}
        ).wait_send()

    with jax.named_scope("sends"):
        send_wait(plane_send, tok.at[pl.ds(0, group - rows)])
        send_wait(cot_send, cot.at[pl.ds(0, group * nr - rows)])
        for q in range(1, nr):
            @pl.when(r + 1 == q)
            def _():
                send_wait(up_send, tok.at[pl.ds(0, q * group)])

            @pl.when(nr - r == q)
            def _():
                send_wait(down_send, tok.at[pl.ds(0, q * group)])

    with jax.named_scope("ywlate"):
        cot_wait(planes[nr - 2], 1)
        cot_wait(planes[nr - 1], 1)


def finish_kernel(x_ref, cot_ref, right_ref, part_ref, out_ref, y, out, sem):
    width, group = x_ref.shape
    total, order = cot_ref.shape[0], right_ref.shape[1]
    step = tile_of(width, FM)
    stores = []
    for b in range(right_ref.shape[0]):
        inside = slice(b * order, (b + 1) * order)
        y[:, inside] = jnp.dot(
            cot_ref[total - group:, inside], right_ref[b], preferred_element_type=jnp.float32
        ).astype(y.dtype)
        for i in range(width // step):
            part = slice(i * step, (i + 1) * step)
            out[part, inside] = (
                part_ref[part, inside]
                + jnp.dot(x_ref[part, :], y[:, inside], preferred_element_type=jnp.float32)
            ).astype(out.dtype)
            stores.append(
                pltpu.make_async_copy(out.at[part, inside], out_ref.at[part, inside], sem.at[len(stores)])
            )
            stores[-1].start()
    for store in stores:
        store.wait()


def body(tokens_in, cotangents, left_root, right_root):
    ne, nr = lax.axis_size("expert"), lax.axis_size("replica")
    assert left_root.shape[0] == 1
    width = tokens_in.shape[1]
    columns = cotangents.shape[1] // nr
    total = tokens_in.shape[0] * nr
    group = tokens_in.shape[0]
    blocks, order = right_root.shape[1], right_root.shape[2]
    anywhere = pl.BlockSpec(memory_space=pl.ANY)
    vmem = pl.BlockSpec(memory_space=pltpu.VMEM)
    dtype = jnp.bfloat16
    dma = pltpu.SemaphoreType.DMA
    regular = pltpu.SemaphoreType.REGULAR
    kept = pl.pallas_call(
        functools.partial(route_kernel, ne, nr),
        out_shape=[
            pltpu.VMEM((width, group), dtype),
            pltpu.VMEM((total, columns), dtype),
            pltpu.VMEM((blocks, order, order), dtype),
            pltpu.VMEM((width, columns), jnp.float32),
        ],
        in_specs=[anywhere] * 4,
        out_specs=[vmem] * 4,
        scratch_shapes=[
            pltpu.VMEM((total, width), dtype),
            pltpu.VMEM((width, width), dtype),
            pltpu.VMEM((width, total - group), dtype),
            pltpu.VMEM((total - group, columns), dtype),
            regular((nr - 1,)), regular((nr - 1,)),
            dma, dma, dma, dma, dma((ne * nr,)), dma((2 * nr,)), dma((2,)),
        ],
        compiler_params=pltpu.CompilerParams(
            collective_id=0, has_side_effects=True, vmem_limit_bytes=34 * 1024 * 1024
        ),
    )(tokens_in, cotangents, left_root[0], right_root[0])
    out = pl.pallas_call(
        finish_kernel,
        out_shape=jax.ShapeDtypeStruct((width, columns), dtype),
        in_specs=[vmem] * 4,
        out_specs=anywhere,
        scratch_shapes=[
            pltpu.VMEM((group, columns), dtype), pltpu.VMEM((width, columns), dtype),
            dma((blocks * (width // tile_of(width, FM)),)),
        ],
        compiler_params=pltpu.CompilerParams(vmem_limit_bytes=16 * 1024 * 1024),
    )(*kept)
    return out[None]


def solution(mesh):
    in_specs = (
        P(("expert", "replica"), None),
        P(("expert", "replica"), None),
        P("expert", None, None),
        P("expert", "replica", None, None),
    )
    out_specs = P("expert", None, "replica")
    return jax.shard_map(body, mesh=mesh, in_specs=in_specs, out_specs=out_specs, check_vma=False)
```

```python
import functools
import jax
import jax.numpy as jnp
from jax import lax
from jax.experimental import pallas as pl
from jax.experimental.pallas import tpu as pltpu
from jax.sharding import PartitionSpec as P

LEAD, C1, C2, AHEAD = 1, 0, 1, 1
XM, PN, FM = 1024, 256, 256


def tile_of(size, most):
    return most if size % most == 0 else size


def route_kernel(
    ne, nr, tok_ref, cot_ref, left_ref, right_ref, x_late, cot, right, done, part_ref,
    tok, left, x, y, low, high,
    plane_send, up_send, down_send, cot_send, tok_recv, cot_recv, local,
):
    e = lax.axis_index("expert")
    r = lax.axis_index("replica")
    rows = tok_ref.shape[0] // ne
    group = rows * ne
    half = group // 2
    width = tok.shape[1]
    cols = cot.shape[1]
    blocks, order = right_ref.shape[0], right_ref.shape[1]

    nc = 2 if ne % 2 == 0 else 1
    nx = 2 if ne % (2 * nc) == 0 else 1
    ny = ne // (nc * nx)
    core = e % nc
    self_k = core * (nx * ny - 1)

    def target_of(k):
        dx, dy, dc = k + core, k // nx + core, k // (nx * ny)
        return ((e // (nc * nx) + dy) % ny * nx + (e // nc + dx) % nx) * nc + (core + dc) % nc

    def at_rows(start, size):
        return pl.ds(pl.multiple_of(start, rows), size)

    def tok_at(origin, k):
        return at_rows((origin * ne + k) * rows, rows)

    def place(tr, origin):
        return jnp.where(tr >= nr // 2, origin + nr - tr, tr + nr - origin) % nr

    def cot_at(tr, origin, k):
        i = place(tr, origin)
        second = k // (ne // 2)
        split = (nr - 2) * group + second * group + (i - (nr - 2)) * half + (k - second * (ne // 2)) * rows
        return at_rows(jnp.where(i < nr - 2, i * group + k * rows, split), rows)

    def own_rows(target):
        return at_rows(target * rows, rows)

    def own_cols(target):
        return pl.ds(pl.multiple_of(target * cols, cols), cols)

    def plane_copy(k):
        target = target_of(k)
        return pltpu.make_async_remote_copy(
            tok_ref.at[own_rows(target)], tok.at[tok_at(r, k)],
            plane_send, tok_recv.at[r * ne + k],
            device_id={"expert": target, "replica": r},
        )

    def relay(origin, k, up, src):
        return pltpu.make_async_remote_copy(
            src, tok.at[tok_at(origin, k)],
            up_send if up else down_send, tok_recv.at[origin * ne + k],
            device_id={"expert": e, "replica": r + 1 if up else r - 1},
        )

    def forward(origin, k, up, src):
        ahead = (r + 1 < nr) if up else (r > 0)

        @pl.when(ahead)
        def _():
            relay(origin, k, up, src).start()

    def tok_wait(origin, k):
        pltpu.make_async_remote_copy(
            tok.at[tok_at(origin, k)], tok.at[tok_at(origin, k)],
            up_send, tok_recv.at[origin * ne + k],
            device_id={"expert": e, "replica": (r + 1) % nr},
        ).wait_recv()

    first = cols - order
    whole_piece, first_blocks, last_block = (0, cols), (0, first), (first, order)

    def cot_copy(k, tr, columns, sem):
        te = target_of(k)
        start, size = columns
        return pltpu.make_async_remote_copy(
            cot_ref.at[own_rows(te), pl.ds(pl.multiple_of(tr * cols + start, order), size)],
            cot.at[cot_at(tr, r, k), pl.ds(start, size)],
            cot_send, cot_recv.at[r * 3 + sem],
            device_id={"expert": te, "replica": tr},
        )

    def send_piece(k, tr):
        @pl.when(k < ne // 2)
        def _():
            cot_copy(k, tr, whole_piece, 0).start()

        @pl.when(k >= ne // 2)
        def _():
            if first:
                cot_copy(k, tr, first_blocks, 1).start()

            @pl.when(place(tr, r) < nr - 2)
            def _():
                cot_copy(k, tr, last_block, 2).start()

    def send_last_block(k, tr):
        @pl.when(place(tr, r) >= nr - 2)
        def _():
            cot_copy(k, tr, last_block, 2).start()

    def cot_wait(origin, sem):
        start, size = (whole_piece, first_blocks, last_block)[sem]
        if size:
            piece = cot.at[pl.ds(0, half), pl.ds(start, size)]
            pltpu.make_async_remote_copy(
                piece, piece, cot_send, cot_recv.at[origin * 3 + sem],
                device_id={"expert": e, "replica": (r + 1) % nr},
            ).wait_recv()

    barrier = pltpu.get_barrier_semaphore()
    above, below = r + 1 < nr, r > 0

    @pl.loop(1, ne)
    def _(k):
        pl.semaphore_signal(barrier, inc=1, device_id={"expert": (e + k) % ne, "replica": r})

    def tell(up, sem):
        @pl.when(above if up else below)
        def _():
            pl.semaphore_signal(sem, inc=1, device_id={"expert": e, "replica": r + 1 if up else r - 1})

    tell(True, barrier)
    tell(False, barrier)

    own_tok = tok_ref.at[own_rows(e)]
    pltpu.make_async_copy(own_tok, tok.at[tok_at(r, self_k)], tok_recv.at[r * ne + self_k]).start()
    pltpu.make_async_copy(
        cot_ref.at[own_rows(e), own_cols(r)], cot.at[cot_at(r, r, self_k)], cot_recv.at[r * 3]
    ).start()
    load_left = pltpu.make_async_copy(left_ref, left, local.at[0])
    load_right = pltpu.make_async_copy(right_ref, right, local.at[1])
    load_left.start()
    load_right.start()
    with jax.named_scope("bar"):
        pl.semaphore_wait(barrier, ne - 1 + above.astype(jnp.int32) + below.astype(jnp.int32))
    tell(True, low.at[0])
    tell(False, high.at[0])

    @pl.loop(0, ne)
    def _(k):
        @pl.when(k != self_k)
        def _():
            plane_copy(k).start()

    def send_cots(k, distance, send=send_piece):
        for tr in (r + distance, r - distance):
            @pl.when((tr >= 0) & (tr < nr))
            def _():
                send(k, tr)

    lag = AHEAD * (nr - 2)

    def send_targets(begin, end, send=send_piece, k0=0):
        @pl.loop(begin, end)
        def _(step):
            def send_all(distances):
                for distance in distances:
                    k = k0 + step - AHEAD * (nr - 1 - distance)
                    ok = (k >= k0) & (k < ne)

                    @pl.when(ok & (k != self_k) if distance == 1 else ok)
                    def _():
                        send_cots(k, distance, send)

            @pl.when(core == 0)
            def _():
                send_all(range(nr - 1, 0, -1))

            @pl.when(core != 0)
            def _():
                send_all(range(1, nr))

    forward(r, self_k, True, own_tok)
    forward(r, self_k, False, own_tok)
    send_cots(self_k, 1)

    with jax.named_scope("ready"):
        for distance in range(1, nr):
            @pl.when(r >= distance)
            def _():
                pl.semaphore_wait(low.at[distance - 1], 1)
                if distance + 1 < nr:
                    tell(True, low.at[distance])

            @pl.when(r + distance < nr)
            def _():
                pl.semaphore_wait(high.at[distance - 1], 1)
                if distance + 1 < nr:
                    tell(False, high.at[distance])

    send_targets(0, LEAD)

    with jax.named_scope("plane"):
        @pl.loop(0, ne)
        def _(k):
            @pl.when(k != self_k)
            def _():
                tok_wait(r, k)
                forward(r, k, True, tok.at[tok_at(r, k)])
                forward(r, k, False, tok.at[tok_at(r, k)])

    def relay_step(distance, k):
        for origin, up in ((r - distance, True), (r + distance, False)):
            @pl.when((origin >= 0) & (origin < nr))
            def _():
                tok_wait(origin, k)
                forward(origin, k, up, tok.at[tok_at(origin, k)])

    sent = LEAD
    for distance in range(1, nr - 1):
        more = (C1, C2)[distance - 1] if distance < 3 else 0
        with jax.named_scope("relay%d" % distance):
            @pl.loop(0, ne)
            def _(k):
                relay_step(distance, k)

                if distance == 1:
                    @pl.when(k != self_k)
                    def _():
                        send_piece(k, r)

                if more:
                    @pl.when(k < more)
                    def _():
                        send_targets(sent + k, sent + k + 1)
        sent += more

    send_targets(sent, ne + lag)
    send_targets(0, ne // 2 + lag, send_last_block, ne // 2)

    planes = [jnp.where(r >= nr // 2, r + i, r + nr - i) % nr for i in range(nr)]

    with jax.named_scope("relay%d" % (nr - 1)):
        @pl.loop(0, ne)
        def _(k):
            relay_step(nr - 1, k)

    load_left.wait()
    tok_wait(r, self_k)
    step = tile_of(width, XM)
    for i, g in enumerate(planes):
        with jax.named_scope("x%d" % i):
            @pl.loop(0, width // step)
            def _(j):
                part = pl.ds(pl.multiple_of(j * step, step), step)
                columns = pl.ds(pl.multiple_of(g * group, group), group)
                tile = lax.dot_general(
                    left[part, :], tok[columns, :], (((1,), (1,)), ((), ())),
                    preferred_element_type=jnp.float32,
                ).astype(x.dtype)
                if i < nr - 2:
                    x[part, i * group:(i + 1) * group] = tile
                else:
                    at = (i - (nr - 2)) * half
                    x[part, (nr - 2) * group + at:(nr - 2) * group + at + half] = tile[:, :half]
                    x_late[part, at:at + half] = tile[:, half:]

    load_right.wait()

    def make_y(begin, blocks_of):
        for b in blocks_of:
            inside = slice(b * order, (b + 1) * order)
            y[begin:begin + group, inside] = jnp.dot(
                cot[begin:begin + group, inside], right[b], preferred_element_type=jnp.float32
            ).astype(y.dtype)

    early = (nr - 1) * group
    for i in range(nr - 2):
        with jax.named_scope("yw%d" % i):
            for sem in range(3):
                cot_wait(planes[i], sem)
        make_y(i * group, range(blocks))

    with jax.named_scope("ywhalf"):
        cot_wait(planes[nr - 2], 0)
        cot_wait(planes[nr - 1], 0)
    make_y(early - group, range(blocks))

    with jax.named_scope("P"):
        step = tile_of(order, PN)

        @pl.loop(0, order // step)
        def _(j):
            at = pl.multiple_of(j * step, step)
            part_ref[:, pl.ds(at, step)] = jnp.dot(
                x[...], y[:early, pl.ds(first + at, step)], preferred_element_type=jnp.float32
            )

    def send_wait(sem, data):
        pltpu.make_async_remote_copy(
            data, data, sem, tok_recv.at[0], device_id={"expert": e, "replica": (r + 1) % nr}
        ).wait_send()

    if first:
        with jax.named_scope("ywfirst"):
            cot_wait(planes[nr - 2], 1)
            cot_wait(planes[nr - 1], 1)
        make_y(early, range(blocks - 1))

        with jax.named_scope("done"):
            @pl.loop(0, first // step)
            def _(j):
                at = pl.ds(pl.multiple_of(j * step, step), step)
                done[:, at] = (
                    jnp.dot(x[...], y[:early, at], preferred_element_type=jnp.float32)
                    + jnp.dot(x_late[...], y[early:, at], preferred_element_type=jnp.float32)
                ).astype(done.dtype)

    with jax.named_scope("sends"):
        send_wait(plane_send, tok.at[pl.ds(0, group - rows)])
        send_wait(cot_send, cot.at[pl.ds(0, group * nr - rows)])
        for q in range(1, nr):
            @pl.when(r + 1 == q)
            def _():
                send_wait(up_send, tok.at[pl.ds(0, q * group)])

            @pl.when(nr - r == q)
            def _():
                send_wait(down_send, tok.at[pl.ds(0, q * group)])

    with jax.named_scope("ywlate"):
        cot_wait(planes[nr - 2], 2)
        cot_wait(planes[nr - 1], 2)


def finish_kernel(x_ref, cot_ref, right_ref, done_ref, part_ref, out_ref, y, out, sem):
    width, group = x_ref.shape
    total, order = cot_ref.shape[0], right_ref.shape[1]
    blocks = right_ref.shape[0]
    first = (blocks - 1) * order
    inside = slice(first, first + order)
    step = tile_of(width, FM)
    stores = []

    def store(data, at, columns):
        stores.append(pltpu.make_async_copy(data, out_ref.at[at, columns], sem.at[len(stores)]))
        stores[-1].start()

    tiles = [slice(i * step, (i + 1) * step) for i in range(width // step)]
    if first:
        for at in tiles:
            store(done_ref.at[at], at, slice(0, first))
    y[...] = jnp.dot(
        cot_ref[total - group:, inside], right_ref[blocks - 1], preferred_element_type=jnp.float32
    ).astype(y.dtype)
    for at in tiles:
        out[at, :] = (
            part_ref[at, :] + jnp.dot(x_ref[at, :], y[...], preferred_element_type=jnp.float32)
        ).astype(out.dtype)
        store(out.at[at], at, inside)
    for copy in stores:
        copy.wait()


def body(tokens_in, cotangents, left_root, right_root):
    ne, nr = lax.axis_size("expert"), lax.axis_size("replica")
    assert left_root.shape[0] == 1
    width = tokens_in.shape[1]
    columns = cotangents.shape[1] // nr
    total = tokens_in.shape[0] * nr
    group = tokens_in.shape[0]
    blocks, order = right_root.shape[1], right_root.shape[2]
    anywhere = pl.BlockSpec(memory_space=pl.ANY)
    vmem = pl.BlockSpec(memory_space=pltpu.VMEM)
    dtype = jnp.bfloat16
    dma = pltpu.SemaphoreType.DMA
    regular = pltpu.SemaphoreType.REGULAR
    kept = pl.pallas_call(
        functools.partial(route_kernel, ne, nr),
        out_shape=[
            pltpu.VMEM((width, group), dtype),
            pltpu.VMEM((total, columns), dtype),
            pltpu.VMEM((blocks, order, order), dtype),
            pltpu.VMEM((width, max(columns - order, 128)), dtype),
            pltpu.VMEM((width, order), jnp.float32),
        ],
        in_specs=[anywhere] * 4,
        out_specs=[vmem] * 5,
        scratch_shapes=[
            pltpu.VMEM((total, width), dtype),
            pltpu.VMEM((width, width), dtype),
            pltpu.VMEM((width, total - group), dtype),
            pltpu.VMEM((total, columns), dtype),
            regular((nr - 1,)), regular((nr - 1,)),
            dma, dma, dma, dma, dma((ne * nr,)), dma((3 * nr,)), dma((2,)),
        ],
        compiler_params=pltpu.CompilerParams(
            collective_id=0, has_side_effects=True, vmem_limit_bytes=34 * 1024 * 1024
        ),
    )(tokens_in, cotangents, left_root[0], right_root[0])
    out = pl.pallas_call(
        finish_kernel,
        out_shape=jax.ShapeDtypeStruct((width, columns), dtype),
        in_specs=[vmem] * 5,
        out_specs=anywhere,
        scratch_shapes=[
            pltpu.VMEM((group, order), dtype), pltpu.VMEM((width, order), dtype),
            dma((2 * (width // tile_of(width, FM)),)),
        ],
        compiler_params=pltpu.CompilerParams(vmem_limit_bytes=16 * 1024 * 1024),
    )(*kept)
    return out[None]


def solution(mesh):
    in_specs = (
        P(("expert", "replica"), None),
        P(("expert", "replica"), None),
        P("expert", None, None),
        P("expert", "replica", None, None),
    )
    out_specs = P("expert", None, "replica")
    return jax.shard_map(body, mesh=mesh, in_specs=in_specs, out_specs=out_specs, check_vma=False)
```

```python
import functools
import jax
import jax.numpy as jnp
from jax import lax
from jax.experimental import pallas as pl
from jax.experimental.pallas import tpu as pltpu
from jax.sharding import PartitionSpec as P

LEAD, C1, C2, AHEAD, PRE = 1, 0, 1, 1, (1,)
XM, PN, FM = 1024, 256, 256


def tile_of(size, most):
    return most if size % most == 0 else size


def plane_of(ne):
    nc = 2 if ne % 2 == 0 else 1
    nx = 2 if ne % (2 * nc) == 0 else 1
    return nc, nx, ne // (nc * nx)


def rounds_of(ne):
    nc, nx, ny = plane_of(ne)
    return max((nc > 1) + (nx > 1) + ny // 2 - 1, 1)


def route_kernel(
    ne, nr, tok_ref, cot_ref, left_ref, right_ref, x_late, cot, right, done, part_ref,
    tok, left, x, y, word, low, high,
    plane_send, up_send, down_send, cot_send, tok_recv, cot_recv, local,
):
    e = lax.axis_index("expert")
    r = lax.axis_index("replica")
    rows = tok_ref.shape[0] // ne
    group = rows * ne
    half = group // 2
    width = tok.shape[1]
    cols = cot.shape[1]
    blocks, order = right_ref.shape[0], right_ref.shape[1]

    nc, nx, ny = plane_of(ne)
    core = e % nc
    self_k = core * (nx * ny - 1)

    def expert_at(dc, dx, dy):
        return ((e // (nc * nx) + dy) % ny * nx + (e // nc + dx) % nx) * nc + (e + dc) % nc

    def target_of(k):
        return expert_at(k // (nx * ny), k + core, k // nx + core)

    def at_rows(start, size):
        return pl.ds(pl.multiple_of(start, rows), size)

    def tok_at(origin, k):
        return at_rows((origin * ne + k) * rows, rows)

    def place(tr, origin):
        return jnp.where(tr >= nr // 2, origin + nr - tr, tr + nr - origin) % nr

    def cot_at(tr, origin, k):
        i = place(tr, origin)
        second = k // (ne // 2)
        split = (nr - 2) * group + second * group + (i - (nr - 2)) * half + (k - second * (ne // 2)) * rows
        return at_rows(jnp.where(i < nr - 2, i * group + k * rows, split), rows)

    def own_rows(target):
        return at_rows(target * rows, rows)

    def own_cols(target):
        return pl.ds(pl.multiple_of(target * cols, cols), cols)

    def plane_copy(k):
        target = target_of(k)
        return pltpu.make_async_remote_copy(
            tok_ref.at[own_rows(target)], tok.at[tok_at(r, k)],
            plane_send, tok_recv.at[r * ne + k],
            device_id={"expert": target, "replica": r},
        )

    def relay(origin, k, up, src):
        return pltpu.make_async_remote_copy(
            src, tok.at[tok_at(origin, k)],
            up_send if up else down_send, tok_recv.at[origin * ne + k],
            device_id={"expert": e, "replica": r + 1 if up else r - 1},
        )

    def forward(origin, k, up, src):
        ahead = (r + 1 < nr) if up else (r > 0)

        @pl.when(ahead)
        def _():
            relay(origin, k, up, src).start()

    def tok_wait(origin, k):
        pltpu.make_async_remote_copy(
            tok.at[tok_at(origin, k)], tok.at[tok_at(origin, k)],
            up_send, tok_recv.at[origin * ne + k],
            device_id={"expert": e, "replica": (r + 1) % nr},
        ).wait_recv()

    first = cols - order
    whole_piece, first_blocks, last_block = (0, cols), (0, first), (first, order)

    def cot_copy(k, tr, columns, sem):
        te = target_of(k)
        start, size = columns
        return pltpu.make_async_remote_copy(
            cot_ref.at[own_rows(te), pl.ds(pl.multiple_of(tr * cols + start, order), size)],
            cot.at[cot_at(tr, r, k), pl.ds(start, size)],
            cot_send, cot_recv.at[r * 3 + sem],
            device_id={"expert": te, "replica": tr},
        )

    def send_piece(k, tr):
        @pl.when(k < ne // 2)
        def _():
            cot_copy(k, tr, whole_piece, 0).start()

        @pl.when(k >= ne // 2)
        def _():
            if first:
                cot_copy(k, tr, first_blocks, 1).start()

            @pl.when(place(tr, r) < nr - 2)
            def _():
                cot_copy(k, tr, last_block, 2).start()

    def send_last_block(k, tr):
        @pl.when(place(tr, r) >= nr - 2)
        def _():
            cot_copy(k, tr, last_block, 2).start()

    def cot_wait(origin, sem):
        start, size = (whole_piece, first_blocks, last_block)[sem]
        if size:
            piece = cot.at[pl.ds(0, half), pl.ds(start, size)]
            pltpu.make_async_remote_copy(
                piece, piece, cot_send, cot_recv.at[origin * 3 + sem],
                device_id={"expert": e, "replica": (r + 1) % nr},
            ).wait_recv()

    barrier = pltpu.get_barrier_semaphore()
    above, below = r + 1 < nr, r > 0

    sides = [(1, 0, 0)] * (nc > 1) + [(0, 1, 0)] * (nx > 1) + [(0, 0, dy) for dy in sorted({1, ny - 1} - {0})]
    rounds = word.shape[0]

    def tell_sides(sem):
        for side in sides:
            pl.semaphore_signal(sem, inc=1, device_id={"expert": expert_at(*side), "replica": r})

    tell_sides(barrier)

    def tell(up, sem):
        @pl.when(above if up else below)
        def _():
            pl.semaphore_signal(sem, inc=1, device_id={"expert": e, "replica": r + 1 if up else r - 1})

    tell(True, barrier)
    tell(False, barrier)

    own_tok = tok_ref.at[own_rows(e)]
    pltpu.make_async_copy(own_tok, tok.at[tok_at(r, self_k)], tok_recv.at[r * ne + self_k]).start()
    pltpu.make_async_copy(
        cot_ref.at[own_rows(e), own_cols(r)], cot.at[cot_at(r, r, self_k)], cot_recv.at[r * 3]
    ).start()
    load_left = pltpu.make_async_copy(left_ref, left, local.at[0])
    load_right = pltpu.make_async_copy(right_ref, right, local.at[1])
    load_left.start()
    load_right.start()
    with jax.named_scope("bar"):
        pl.semaphore_wait(barrier, len(sides) + above.astype(jnp.int32) + below.astype(jnp.int32))

    def send_cots(k, distance, send=send_piece):
        for tr in (r + distance, r - distance):
            @pl.when((tr >= 0) & (tr < nr))
            def _():
                send(k, tr)

    lag = AHEAD * (nr - 2)
    pre = PRE

    def send_targets(begin, end, send=send_piece, k0=0, order_of=lambda k: k):
        @pl.loop(begin, end)
        def _(step):
            def send_all(distances):
                for distance in distances:
                    k = step - AHEAD * (nr - 1 - distance)
                    ok = (k >= 0) & (k < ne - k0)
                    k = order_of(k) + k0

                    if distance == 1:
                        ok &= k != self_k
                        for sent_k in pre if k0 == 0 else ():
                            ok &= k != sent_k

                    @pl.when(ok)
                    def _():
                        send_cots(k, distance, send)

            @pl.when(core == 0)
            def _():
                send_all(range(nr - 1, 0, -1))

            @pl.when(core != 0)
            def _():
                send_all(range(1, nr))

    forward(r, self_k, True, own_tok)
    forward(r, self_k, False, own_tok)
    send_cots(self_k, 1)

    with jax.named_scope("rounds"):
        for t in range(rounds):
            tell_sides(word.at[t])
            pl.semaphore_wait(word.at[t], len(sides))
        tell(True, low.at[0])
        tell(False, high.at[0])

    @pl.loop(0, ne)
    def _(k):
        @pl.when(k != self_k)
        def _():
            plane_copy(k).start()

    with jax.named_scope("ready"):
        for distance in range(1, nr):
            @pl.when(r >= distance)
            def _():
                pl.semaphore_wait(low.at[distance - 1], 1)
                if distance + 1 < nr:
                    tell(True, low.at[distance])

            @pl.when(r + distance < nr)
            def _():
                pl.semaphore_wait(high.at[distance - 1], 1)
                if distance + 1 < nr:
                    tell(False, high.at[distance])

            if distance == 1:
                for k in pre:
                    send_cots(k, 1)

    send_targets(0, LEAD)

    with jax.named_scope("plane"):
        @pl.loop(0, ne)
        def _(k):
            @pl.when(k != self_k)
            def _():
                tok_wait(r, k)
                forward(r, k, True, tok.at[tok_at(r, k)])
                forward(r, k, False, tok.at[tok_at(r, k)])

    def relay_step(distance, k):
        for origin, up in ((r - distance, True), (r + distance, False)):
            @pl.when((origin >= 0) & (origin < nr))
            def _():
                tok_wait(origin, k)
                forward(origin, k, up, tok.at[tok_at(origin, k)])

    def own_column_last(k):
        turned = jnp.where(k < ne // 4, k + ne // 4, ne // 2 - 1 - k)
        return jnp.where(core == 0, turned, k)

    sent = LEAD
    for distance in range(1, nr - 1):
        more = (C1, C2)[distance - 1] if distance < 3 else 0
        with jax.named_scope("relay%d" % distance):
            @pl.loop(0, ne)
            def _(k):
                relay_step(distance, k)

                if distance == 1:
                    @pl.when(k != self_k)
                    def _():
                        send_piece(k, r)

                if more:
                    @pl.when(k < more)
                    def _():
                        send_targets(sent + k, sent + k + 1)
        sent += more

    send_targets(sent, ne + lag)
    send_targets(0, ne // 2 + lag, send_last_block, ne // 2, own_column_last)

    planes = [jnp.where(r >= nr // 2, r + i, r + nr - i) % nr for i in range(nr)]

    with jax.named_scope("relay%d" % (nr - 1)):
        @pl.loop(0, ne)
        def _(k):
            relay_step(nr - 1, k)

    load_left.wait()
    tok_wait(r, self_k)
    step = tile_of(width, XM)
    for i, g in enumerate(planes):
        with jax.named_scope("x%d" % i):
            @pl.loop(0, width // step)
            def _(j):
                part = pl.ds(pl.multiple_of(j * step, step), step)
                columns = pl.ds(pl.multiple_of(g * group, group), group)
                tile = lax.dot_general(
                    left[part, :], tok[columns, :], (((1,), (1,)), ((), ())),
                    preferred_element_type=jnp.float32,
                ).astype(x.dtype)
                if i < nr - 2:
                    x[part, i * group:(i + 1) * group] = tile
                else:
                    at = (i - (nr - 2)) * half
                    x[part, (nr - 2) * group + at:(nr - 2) * group + at + half] = tile[:, :half]
                    x_late[part, at:at + half] = tile[:, half:]

    load_right.wait()

    def make_y(begin, blocks_of):
        for b in blocks_of:
            inside = slice(b * order, (b + 1) * order)
            y[begin:begin + group, inside] = jnp.dot(
                cot[begin:begin + group, inside], right[b], preferred_element_type=jnp.float32
            ).astype(y.dtype)

    early = (nr - 1) * group
    for i in range(nr - 2):
        with jax.named_scope("yw%d" % i):
            for sem in range(3):
                cot_wait(planes[i], sem)
        make_y(i * group, range(blocks))

    with jax.named_scope("ywhalf"):
        cot_wait(planes[nr - 2], 0)
        cot_wait(planes[nr - 1], 0)
    make_y(early - group, range(blocks))

    with jax.named_scope("P"):
        step = tile_of(order, PN)

        @pl.loop(0, order // step)
        def _(j):
            at = pl.multiple_of(j * step, step)
            part_ref[:, pl.ds(at, step)] = jnp.dot(
                x[...], y[:early, pl.ds(first + at, step)], preferred_element_type=jnp.float32
            )

    def send_wait(sem, data):
        pltpu.make_async_remote_copy(
            data, data, sem, tok_recv.at[0], device_id={"expert": e, "replica": (r + 1) % nr}
        ).wait_send()

    if first:
        with jax.named_scope("ywfirst"):
            cot_wait(planes[nr - 2], 1)
            cot_wait(planes[nr - 1], 1)
        make_y(early, range(blocks - 1))

        with jax.named_scope("done"):
            @pl.loop(0, first // step)
            def _(j):
                at = pl.ds(pl.multiple_of(j * step, step), step)
                done[:, at] = (
                    jnp.dot(x[...], y[:early, at], preferred_element_type=jnp.float32)
                    + jnp.dot(x_late[...], y[early:, at], preferred_element_type=jnp.float32)
                ).astype(done.dtype)

    with jax.named_scope("sends"):
        send_wait(plane_send, tok.at[pl.ds(0, group - rows)])
        send_wait(cot_send, cot.at[pl.ds(0, group * nr - rows)])
        for q in range(1, nr):
            @pl.when(r + 1 == q)
            def _():
                send_wait(up_send, tok.at[pl.ds(0, q * group)])

            @pl.when(nr - r == q)
            def _():
                send_wait(down_send, tok.at[pl.ds(0, q * group)])

    with jax.named_scope("ywlate"):
        cot_wait(planes[nr - 2], 2)
        cot_wait(planes[nr - 1], 2)


def finish_kernel(x_ref, cot_ref, right_ref, done_ref, part_ref, out_ref, y, out, sem):
    width, group = x_ref.shape
    total, order = cot_ref.shape[0], right_ref.shape[1]
    blocks = right_ref.shape[0]
    first = (blocks - 1) * order
    inside = slice(first, first + order)
    step = tile_of(width, FM)
    stores = []

    def store(data, at, columns):
        stores.append(pltpu.make_async_copy(data, out_ref.at[at, columns], sem.at[len(stores)]))
        stores[-1].start()

    tiles = [slice(i * step, (i + 1) * step) for i in range(width // step)]
    if first:
        for at in tiles:
            store(done_ref.at[at], at, slice(0, first))
    y[...] = jnp.dot(
        cot_ref[total - group:, inside], right_ref[blocks - 1], preferred_element_type=jnp.float32
    ).astype(y.dtype)
    for at in tiles:
        out[at, :] = (
            part_ref[at, :] + jnp.dot(x_ref[at, :], y[...], preferred_element_type=jnp.float32)
        ).astype(out.dtype)
        store(out.at[at], at, inside)
    for copy in stores:
        copy.wait()


def body(tokens_in, cotangents, left_root, right_root):
    ne, nr = lax.axis_size("expert"), lax.axis_size("replica")
    assert left_root.shape[0] == 1
    width = tokens_in.shape[1]
    columns = cotangents.shape[1] // nr
    total = tokens_in.shape[0] * nr
    group = tokens_in.shape[0]
    blocks, order = right_root.shape[1], right_root.shape[2]
    anywhere = pl.BlockSpec(memory_space=pl.ANY)
    vmem = pl.BlockSpec(memory_space=pltpu.VMEM)
    dtype = jnp.bfloat16
    dma = pltpu.SemaphoreType.DMA
    regular = pltpu.SemaphoreType.REGULAR
    kept = pl.pallas_call(
        functools.partial(route_kernel, ne, nr),
        out_shape=[
            pltpu.VMEM((width, group), dtype),
            pltpu.VMEM((total, columns), dtype),
            pltpu.VMEM((blocks, order, order), dtype),
            pltpu.VMEM((width, max(columns - order, 128)), dtype),
            pltpu.VMEM((width, order), jnp.float32),
        ],
        in_specs=[anywhere] * 4,
        out_specs=[vmem] * 5,
        scratch_shapes=[
            pltpu.VMEM((total, width), dtype),
            pltpu.VMEM((width, width), dtype),
            pltpu.VMEM((width, total - group), dtype),
            pltpu.VMEM((total, columns), dtype),
            regular((rounds_of(ne),)), regular((nr - 1,)), regular((nr - 1,)),
            dma, dma, dma, dma, dma((ne * nr,)), dma((3 * nr,)), dma((2,)),
        ],
        compiler_params=pltpu.CompilerParams(
            collective_id=0, has_side_effects=True, vmem_limit_bytes=34 * 1024 * 1024
        ),
    )(tokens_in, cotangents, left_root[0], right_root[0])
    out = pl.pallas_call(
        finish_kernel,
        out_shape=jax.ShapeDtypeStruct((width, columns), dtype),
        in_specs=[vmem] * 5,
        out_specs=anywhere,
        scratch_shapes=[
            pltpu.VMEM((group, order), dtype), pltpu.VMEM((width, order), dtype),
            dma((2 * (width // tile_of(width, FM)),)),
        ],
        compiler_params=pltpu.CompilerParams(vmem_limit_bytes=16 * 1024 * 1024),
    )(*kept)
    return out[None]


def solution(mesh):
    in_specs = (
        P(("expert", "replica"), None),
        P(("expert", "replica"), None),
        P("expert", None, None),
        P("expert", "replica", None, None),
    )
    out_specs = P("expert", None, "replica")
    return jax.shard_map(body, mesh=mesh, in_specs=in_specs, out_specs=out_specs, check_vma=False)
```

```python
import functools
import jax
import jax.numpy as jnp
from jax import lax
from jax.experimental import pallas as pl
from jax.experimental.pallas import tpu as pltpu
from jax.sharding import PartitionSpec as P

LEAD, C1, C2, AHEAD, PRE = 2, 0, 2, 1, (1,)
XM, PN, FM = 1024, 256, 256


def tile_of(size, most):
    return most if size % most == 0 else size


def plane_of(ne):
    nc = 2 if ne % 2 == 0 else 1
    nx = 2 if ne % (2 * nc) == 0 else 1
    return nc, nx, ne // (nc * nx)


def rounds_of(ne):
    nc, nx, ny = plane_of(ne)
    return max((nc > 1) + (nx > 1) + ny // 2 - 1, 1)


def route_kernel(
    ne, nr, tok_ref, cot_ref, left_ref, right_ref, x_late, cot, right, done, part_ref,
    tok, left, x, y, word, low, high,
    plane_send, up_send, down_send, cot_send, tok_recv, cot_recv, local,
):
    e = lax.axis_index("expert")
    r = lax.axis_index("replica")
    rows = tok_ref.shape[0] // ne
    group = rows * ne
    half = group // 2
    width = tok.shape[1]
    cols = cot.shape[1]
    blocks, order = right_ref.shape[0], right_ref.shape[1]

    nc, nx, ny = plane_of(ne)
    core = e % nc
    self_k = core * (nx * ny - 1)

    def expert_at(dc, dx, dy):
        return ((e // (nc * nx) + dy) % ny * nx + (e // nc + dx) % nx) * nc + (e + dc) % nc

    def target_of(k):
        return expert_at(k // (nx * ny), k + core, k // nx + core)

    def at_rows(start, size):
        return pl.ds(pl.multiple_of(start, rows), size)

    def tok_at(origin, k):
        return at_rows((origin * ne + k) * rows, rows)

    def place(tr, origin):
        return jnp.where(tr >= nr // 2, origin + nr - tr, tr + nr - origin) % nr

    def cot_at(tr, origin, k):
        i = place(tr, origin)
        second = k // (ne // 2)
        split = (nr - 2) * group + second * group + (i - (nr - 2)) * half + (k - second * (ne // 2)) * rows
        return at_rows(jnp.where(i < nr - 2, i * group + k * rows, split), rows)

    def own_rows(target):
        return at_rows(target * rows, rows)

    def own_cols(target):
        return pl.ds(pl.multiple_of(target * cols, cols), cols)

    def plane_copy(k):
        target = target_of(k)
        return pltpu.make_async_remote_copy(
            tok_ref.at[own_rows(target)], tok.at[tok_at(r, k)],
            plane_send, tok_recv.at[r * ne + k],
            device_id={"expert": target, "replica": r},
        )

    def relay(origin, k, up, src):
        return pltpu.make_async_remote_copy(
            src, tok.at[tok_at(origin, k)],
            up_send if up else down_send, tok_recv.at[origin * ne + k],
            device_id={"expert": e, "replica": r + 1 if up else r - 1},
        )

    def forward(origin, k, up, src):
        ahead = (r + 1 < nr) if up else (r > 0)

        @pl.when(ahead)
        def _():
            relay(origin, k, up, src).start()

    def tok_wait(origin, k):
        pltpu.make_async_remote_copy(
            tok.at[tok_at(origin, k)], tok.at[tok_at(origin, k)],
            up_send, tok_recv.at[origin * ne + k],
            device_id={"expert": e, "replica": (r + 1) % nr},
        ).wait_recv()

    first = cols - order
    whole_piece, first_blocks, last_block = (0, cols), (0, first), (first, order)

    def cot_copy(k, tr, columns, sem):
        te = target_of(k)
        start, size = columns
        return pltpu.make_async_remote_copy(
            cot_ref.at[own_rows(te), pl.ds(pl.multiple_of(tr * cols + start, order), size)],
            cot.at[cot_at(tr, r, k), pl.ds(start, size)],
            cot_send, cot_recv.at[r * 3 + sem],
            device_id={"expert": te, "replica": tr},
        )

    def send_piece(k, tr):
        @pl.when(k < ne // 2)
        def _():
            cot_copy(k, tr, whole_piece, 0).start()

        @pl.when(k >= ne // 2)
        def _():
            if first:
                cot_copy(k, tr, first_blocks, 1).start()

            @pl.when(place(tr, r) < nr - 2)
            def _():
                cot_copy(k, tr, last_block, 2).start()

    def send_last_block(k, tr):
        @pl.when(place(tr, r) >= nr - 2)
        def _():
            cot_copy(k, tr, last_block, 2).start()

    def cot_wait(origin, sem):
        start, size = (whole_piece, first_blocks, last_block)[sem]
        if size:
            piece = cot.at[pl.ds(0, half), pl.ds(start, size)]
            pltpu.make_async_remote_copy(
                piece, piece, cot_send, cot_recv.at[origin * 3 + sem],
                device_id={"expert": e, "replica": (r + 1) % nr},
            ).wait_recv()

    barrier = pltpu.get_barrier_semaphore()
    above, below = r + 1 < nr, r > 0

    sides = [(1, 0, 0)] * (nc > 1) + [(0, 1, 0)] * (nx > 1) + [(0, 0, dy) for dy in sorted({1, ny - 1} - {0})]
    rounds = word.shape[0]

    def tell_sides(sem):
        for side in sides:
            pl.semaphore_signal(sem, inc=1, device_id={"expert": expert_at(*side), "replica": r})

    tell_sides(barrier)

    def tell(up, sem):
        @pl.when(above if up else below)
        def _():
            pl.semaphore_signal(sem, inc=1, device_id={"expert": e, "replica": r + 1 if up else r - 1})

    tell(True, barrier)
    tell(False, barrier)

    own_tok = tok_ref.at[own_rows(e)]
    pltpu.make_async_copy(own_tok, tok.at[tok_at(r, self_k)], tok_recv.at[r * ne + self_k]).start()
    pltpu.make_async_copy(
        cot_ref.at[own_rows(e), own_cols(r)], cot.at[cot_at(r, r, self_k)], cot_recv.at[r * 3]
    ).start()
    load_left = pltpu.make_async_copy(left_ref, left, local.at[0])
    load_right = pltpu.make_async_copy(right_ref, right, local.at[1])
    load_left.start()
    load_right.start()
    with jax.named_scope("bar"):
        pl.semaphore_wait(barrier, len(sides) + above.astype(jnp.int32) + below.astype(jnp.int32))

    def send_cots(k, distance, send=send_piece):
        for tr in (r + distance, r - distance):
            @pl.when((tr >= 0) & (tr < nr))
            def _():
                send(k, tr)

    lag = AHEAD * (nr - 2)
    pre = PRE

    def send_targets(begin, end, send=send_piece, k0=0, order_of=lambda k: k):
        @pl.loop(begin, end)
        def _(step):
            def send_all(distances):
                for distance in distances:
                    k = step - AHEAD * (nr - 1 - distance)
                    ok = (k >= 0) & (k < ne - k0)
                    k = order_of(k) + k0

                    if distance == 1:
                        ok &= k != self_k
                        for sent_k in pre if k0 == 0 else ():
                            ok &= k != sent_k

                    @pl.when(ok)
                    def _():
                        send_cots(k, distance, send)

            @pl.when(core == 0)
            def _():
                send_all(range(nr - 1, 0, -1))

            @pl.when(core != 0)
            def _():
                send_all(range(1, nr))

    forward(r, self_k, True, own_tok)
    forward(r, self_k, False, own_tok)
    send_cots(self_k, 1)

    with jax.named_scope("rounds"):
        for t in range(rounds):
            tell_sides(word.at[t])
            pl.semaphore_wait(word.at[t], len(sides))
        tell(True, low.at[0])
        tell(False, high.at[0])

    @pl.loop(0, ne)
    def _(k):
        @pl.when(k != self_k)
        def _():
            plane_copy(k).start()

    with jax.named_scope("ready"):
        for distance in range(1, nr):
            @pl.when(r >= distance)
            def _():
                pl.semaphore_wait(low.at[distance - 1], 1)
                if distance + 1 < nr:
                    tell(True, low.at[distance])

            @pl.when(r + distance < nr)
            def _():
                pl.semaphore_wait(high.at[distance - 1], 1)
                if distance + 1 < nr:
                    tell(False, high.at[distance])

            if distance == 1:
                for k in pre:
                    send_cots(k, 1)

    send_targets(0, LEAD)

    with jax.named_scope("plane"):
        @pl.loop(0, ne)
        def _(k):
            @pl.when(k != self_k)
            def _():
                tok_wait(r, k)
                forward(r, k, True, tok.at[tok_at(r, k)])
                forward(r, k, False, tok.at[tok_at(r, k)])

    def relay_step(distance, k):
        for origin, up in ((r - distance, True), (r + distance, False)):
            @pl.when((origin >= 0) & (origin < nr))
            def _():
                tok_wait(origin, k)
                forward(origin, k, up, tok.at[tok_at(origin, k)])

    def own_column_last(k):
        k = jnp.where(e // nc == 0, (k + ne // 2 - 1) % (ne // 2), k)
        turned = jnp.where(k < ne // 4, k + ne // 4, ne // 2 - 1 - k)
        return jnp.where(core == 0, turned, k)

    sent = LEAD
    for distance in range(1, nr - 1):
        more = (C1, C2)[distance - 1] if distance < 3 else 0
        with jax.named_scope("relay%d" % distance):
            @pl.loop(0, ne)
            def _(k):
                relay_step(distance, k)

                if distance == 1:
                    @pl.when(k != self_k)
                    def _():
                        send_piece(k, r)

                if more:
                    @pl.when(k < more)
                    def _():
                        send_targets(sent + k, sent + k + 1)
        sent += more

    send_targets(sent, ne + lag)
    send_targets(0, ne // 2 + lag, send_last_block, ne // 2, own_column_last)

    planes = [jnp.where(r >= nr // 2, r + i, r + nr - i) % nr for i in range(nr)]

    with jax.named_scope("relay%d" % (nr - 1)):
        @pl.loop(0, ne)
        def _(k):
            relay_step(nr - 1, k)

    load_left.wait()
    tok_wait(r, self_k)
    step = tile_of(width, XM)
    for i, g in enumerate(planes):
        with jax.named_scope("x%d" % i):
            @pl.loop(0, width // step)
            def _(j):
                part = pl.ds(pl.multiple_of(j * step, step), step)
                columns = pl.ds(pl.multiple_of(g * group, group), group)
                tile = lax.dot_general(
                    left[part, :], tok[columns, :], (((1,), (1,)), ((), ())),
                    preferred_element_type=jnp.float32,
                ).astype(x.dtype)
                if i < nr - 2:
                    x[part, i * group:(i + 1) * group] = tile
                else:
                    at = (i - (nr - 2)) * half
                    x[part, (nr - 2) * group + at:(nr - 2) * group + at + half] = tile[:, :half]
                    x_late[part, at:at + half] = tile[:, half:]

    load_right.wait()

    def make_y(begin, blocks_of):
        for b in blocks_of:
            inside = slice(b * order, (b + 1) * order)
            y[begin:begin + group, inside] = jnp.dot(
                cot[begin:begin + group, inside], right[b], preferred_element_type=jnp.float32
            ).astype(y.dtype)

    early = (nr - 1) * group
    for i in range(nr - 2):
        with jax.named_scope("yw%d" % i):
            for sem in range(3):
                cot_wait(planes[i], sem)
        make_y(i * group, range(blocks))

    with jax.named_scope("ywhalf"):
        cot_wait(planes[nr - 2], 0)
        cot_wait(planes[nr - 1], 0)
    make_y(early - group, range(blocks))

    with jax.named_scope("P"):
        step = tile_of(order, PN)

        @pl.loop(0, order // step)
        def _(j):
            at = pl.multiple_of(j * step, step)
            part_ref[:, pl.ds(at, step)] = jnp.dot(
                x[...], y[:early, pl.ds(first + at, step)], preferred_element_type=jnp.float32
            )

    def send_wait(sem, data):
        pltpu.make_async_remote_copy(
            data, data, sem, tok_recv.at[0], device_id={"expert": e, "replica": (r + 1) % nr}
        ).wait_send()

    if first:
        with jax.named_scope("ywfirst"):
            cot_wait(planes[nr - 2], 1)
            cot_wait(planes[nr - 1], 1)
        make_y(early, range(blocks - 1))

        with jax.named_scope("done"):
            @pl.loop(0, first // step)
            def _(j):
                at = pl.ds(pl.multiple_of(j * step, step), step)
                done[:, at] = (
                    jnp.dot(x[...], y[:early, at], preferred_element_type=jnp.float32)
                    + jnp.dot(x_late[...], y[early:, at], preferred_element_type=jnp.float32)
                ).astype(done.dtype)

    with jax.named_scope("sends"):
        send_wait(plane_send, tok.at[pl.ds(0, group - rows)])
        send_wait(cot_send, cot.at[pl.ds(0, group * nr - rows)])
        for q in range(1, nr):
            @pl.when(r + 1 == q)
            def _():
                send_wait(up_send, tok.at[pl.ds(0, q * group)])

            @pl.when(nr - r == q)
            def _():
                send_wait(down_send, tok.at[pl.ds(0, q * group)])

    with jax.named_scope("ywlate"):
        cot_wait(planes[nr - 2], 2)
        cot_wait(planes[nr - 1], 2)


def finish_kernel(x_ref, cot_ref, right_ref, done_ref, part_ref, out_ref, y, out, sem):
    width, group = x_ref.shape
    total, order = cot_ref.shape[0], right_ref.shape[1]
    blocks = right_ref.shape[0]
    first = (blocks - 1) * order
    inside = slice(first, first + order)
    step = tile_of(width, FM)
    stores = []

    def store(data, at, columns):
        stores.append(pltpu.make_async_copy(data, out_ref.at[at, columns], sem.at[len(stores)]))
        stores[-1].start()

    tiles = [slice(i * step, (i + 1) * step) for i in range(width // step)]
    if first:
        for at in tiles:
            store(done_ref.at[at], at, slice(0, first))
    y[...] = jnp.dot(
        cot_ref[total - group:, inside], right_ref[blocks - 1], preferred_element_type=jnp.float32
    ).astype(y.dtype)
    for at in tiles:
        out[at, :] = (
            part_ref[at, :] + jnp.dot(x_ref[at, :], y[...], preferred_element_type=jnp.float32)
        ).astype(out.dtype)
        store(out.at[at], at, inside)
    for copy in stores:
        copy.wait()


def body(tokens_in, cotangents, left_root, right_root):
    ne, nr = lax.axis_size("expert"), lax.axis_size("replica")
    assert left_root.shape[0] == 1
    width = tokens_in.shape[1]
    columns = cotangents.shape[1] // nr
    total = tokens_in.shape[0] * nr
    group = tokens_in.shape[0]
    blocks, order = right_root.shape[1], right_root.shape[2]
    anywhere = pl.BlockSpec(memory_space=pl.ANY)
    vmem = pl.BlockSpec(memory_space=pltpu.VMEM)
    dtype = jnp.bfloat16
    dma = pltpu.SemaphoreType.DMA
    regular = pltpu.SemaphoreType.REGULAR
    kept = pl.pallas_call(
        functools.partial(route_kernel, ne, nr),
        out_shape=[
            pltpu.VMEM((width, group), dtype),
            pltpu.VMEM((total, columns), dtype),
            pltpu.VMEM((blocks, order, order), dtype),
            pltpu.VMEM((width, max(columns - order, 128)), dtype),
            pltpu.VMEM((width, order), jnp.float32),
        ],
        in_specs=[anywhere] * 4,
        out_specs=[vmem] * 5,
        scratch_shapes=[
            pltpu.VMEM((total, width), dtype),
            pltpu.VMEM((width, width), dtype),
            pltpu.VMEM((width, total - group), dtype),
            pltpu.VMEM((total, columns), dtype),
            regular((rounds_of(ne),)), regular((nr - 1,)), regular((nr - 1,)),
            dma, dma, dma, dma, dma((ne * nr,)), dma((3 * nr,)), dma((2,)),
        ],
        compiler_params=pltpu.CompilerParams(
            collective_id=0, has_side_effects=True, vmem_limit_bytes=34 * 1024 * 1024
        ),
    )(tokens_in, cotangents, left_root[0], right_root[0])
    out = pl.pallas_call(
        finish_kernel,
        out_shape=jax.ShapeDtypeStruct((width, columns), dtype),
        in_specs=[vmem] * 5,
        out_specs=anywhere,
        scratch_shapes=[
            pltpu.VMEM((group, order), dtype), pltpu.VMEM((width, order), dtype),
            dma((2 * (width // tile_of(width, FM)),)),
        ],
        compiler_params=pltpu.CompilerParams(vmem_limit_bytes=16 * 1024 * 1024),
    )(*kept)
    return out[None]


def solution(mesh):
    in_specs = (
        P(("expert", "replica"), None),
        P(("expert", "replica"), None),
        P("expert", None, None),
        P("expert", "replica", None, None),
    )
    out_specs = P("expert", None, "replica")
    return jax.shard_map(body, mesh=mesh, in_specs=in_specs, out_specs=out_specs, check_vma=False)
```

```python
import functools
import jax
import jax.numpy as jnp
from jax import lax
from jax.experimental import pallas as pl
from jax.experimental.pallas import tpu as pltpu
from jax.sharding import PartitionSpec as P

LEAD, C1, C2, AHEAD, PRE = 2, 0, 3, 1, (1,)
XM, PN, FM = 1024, 256, 256


def tile_of(size, most):
    return most if size % most == 0 else size


def plane_of(ne):
    nc = 2 if ne % 2 == 0 else 1
    nx = 2 if ne % (2 * nc) == 0 else 1
    return nc, nx, ne // (nc * nx)


def rounds_of(ne):
    nc, nx, ny = plane_of(ne)
    return max((nc > 1) + (nx > 1) + ny // 2 - 1, 1)


def route_kernel(
    ne, nr, tok_ref, cot_ref, left_ref, right_ref, x_late, cot, right, done, part_ref,
    tok, left, x, y, word, low, high,
    plane_send, up_send, down_send, cot_send, tok_recv, cot_recv, local,
):
    e = lax.axis_index("expert")
    r = lax.axis_index("replica")
    rows = tok_ref.shape[0] // ne
    group = rows * ne
    half = group // 2
    width = tok.shape[1]
    cols = cot.shape[1]
    blocks, order = right_ref.shape[0], right_ref.shape[1]

    nc, nx, ny = plane_of(ne)
    core = e % nc
    self_k = core * (nx * ny - 1)

    def expert_at(dc, dx, dy):
        return ((e // (nc * nx) + dy) % ny * nx + (e // nc + dx) % nx) * nc + (e + dc) % nc

    def target_of(k):
        return expert_at(k // (nx * ny), k + core, k // nx + core)

    def at_rows(start, size):
        return pl.ds(pl.multiple_of(start, rows), size)

    def tok_at(origin, k):
        return at_rows((origin * ne + k) * rows, rows)

    def place(tr, origin):
        return jnp.where(tr >= nr // 2, origin + nr - tr, tr + nr - origin) % nr

    def cot_at(tr, origin, k):
        i = place(tr, origin)
        second = k // (ne // 2)
        split = (nr - 2) * group + second * group + (i - (nr - 2)) * half + (k - second * (ne // 2)) * rows
        return at_rows(jnp.where(i < nr - 2, i * group + k * rows, split), rows)

    def own_rows(target):
        return at_rows(target * rows, rows)

    def own_cols(target):
        return pl.ds(pl.multiple_of(target * cols, cols), cols)

    def plane_copy(k):
        target = target_of(k)
        return pltpu.make_async_remote_copy(
            tok_ref.at[own_rows(target)], tok.at[tok_at(r, k)],
            plane_send, tok_recv.at[r * ne + k],
            device_id={"expert": target, "replica": r},
        )

    def relay(origin, k, up, src):
        return pltpu.make_async_remote_copy(
            src, tok.at[tok_at(origin, k)],
            up_send if up else down_send, tok_recv.at[origin * ne + k],
            device_id={"expert": e, "replica": r + 1 if up else r - 1},
        )

    def forward(origin, k, up, src):
        ahead = (r + 1 < nr) if up else (r > 0)

        @pl.when(ahead)
        def _():
            relay(origin, k, up, src).start()

    def tok_wait(origin, k):
        pltpu.make_async_remote_copy(
            tok.at[tok_at(origin, k)], tok.at[tok_at(origin, k)],
            up_send, tok_recv.at[origin * ne + k],
            device_id={"expert": e, "replica": (r + 1) % nr},
        ).wait_recv()

    first = cols - order
    whole_piece, first_blocks, last_block = (0, cols), (0, first), (first, order)

    def cot_copy(k, tr, columns, sem):
        te = target_of(k)
        start, size = columns
        return pltpu.make_async_remote_copy(
            cot_ref.at[own_rows(te), pl.ds(pl.multiple_of(tr * cols + start, order), size)],
            cot.at[cot_at(tr, r, k), pl.ds(start, size)],
            cot_send, cot_recv.at[r * 3 + sem],
            device_id={"expert": te, "replica": tr},
        )

    def send_piece(k, tr):
        @pl.when(k < ne // 2)
        def _():
            cot_copy(k, tr, whole_piece, 0).start()

        @pl.when(k >= ne // 2)
        def _():
            if first:
                cot_copy(k, tr, first_blocks, 1).start()

            @pl.when(place(tr, r) < nr - 2)
            def _():
                cot_copy(k, tr, last_block, 2).start()

    def send_last_block(k, tr):
        @pl.when(place(tr, r) >= nr - 2)
        def _():
            cot_copy(k, tr, last_block, 2).start()

    def cot_wait(origin, sem):
        start, size = (whole_piece, first_blocks, last_block)[sem]
        if size:
            piece = cot.at[pl.ds(0, half), pl.ds(start, size)]
            pltpu.make_async_remote_copy(
                piece, piece, cot_send, cot_recv.at[origin * 3 + sem],
                device_id={"expert": e, "replica": (r + 1) % nr},
            ).wait_recv()

    barrier = pltpu.get_barrier_semaphore()
    above, below = r + 1 < nr, r > 0

    sides = [(1, 0, 0)] * (nc > 1) + [(0, 1, 0)] * (nx > 1) + [(0, 0, dy) for dy in sorted({1, ny - 1} - {0})]
    rounds = word.shape[0]

    def tell_sides(sem):
        for side in sides:
            pl.semaphore_signal(sem, inc=1, device_id={"expert": expert_at(*side), "replica": r})

    tell_sides(barrier)

    def tell(up, sem):
        @pl.when(above if up else below)
        def _():
            pl.semaphore_signal(sem, inc=1, device_id={"expert": e, "replica": r + 1 if up else r - 1})

    tell(True, barrier)
    tell(False, barrier)

    own_tok = tok_ref.at[own_rows(e)]
    pltpu.make_async_copy(own_tok, tok.at[tok_at(r, self_k)], tok_recv.at[r * ne + self_k]).start()
    pltpu.make_async_copy(
        cot_ref.at[own_rows(e), own_cols(r)], cot.at[cot_at(r, r, self_k)], cot_recv.at[r * 3]
    ).start()
    load_left = pltpu.make_async_copy(left_ref, left, local.at[0])
    load_right = pltpu.make_async_copy(right_ref, right, local.at[1])
    load_left.start()
    load_right.start()
    with jax.named_scope("bar"):
        pl.semaphore_wait(barrier, len(sides) + above.astype(jnp.int32) + below.astype(jnp.int32))

    def send_cots(k, distance, send=send_piece):
        for tr in (r + distance, r - distance):
            @pl.when((tr >= 0) & (tr < nr))
            def _():
                send(k, tr)

    lag = AHEAD * (nr - 2)
    pre = PRE

    def send_targets(begin, end, send=send_piece, k0=0, order_of=lambda k: k):
        @pl.loop(begin, end)
        def _(step):
            def send_all(distances):
                for distance in distances:
                    k = step - AHEAD * (nr - 1 - distance)
                    ok = (k >= 0) & (k < ne - k0)
                    k = order_of(k) + k0

                    if distance == 1:
                        ok &= k != self_k
                        for sent_k in pre if k0 == 0 else ():
                            ok &= k != sent_k

                    @pl.when(ok)
                    def _():
                        send_cots(k, distance, send)

            @pl.when(core == 0)
            def _():
                send_all(range(nr - 1, 0, -1))

            @pl.when(core != 0)
            def _():
                send_all(range(1, nr))

    forward(r, self_k, True, own_tok)
    forward(r, self_k, False, own_tok)
    send_cots(self_k, 1)

    with jax.named_scope("rounds"):
        for t in range(rounds):
            tell_sides(word.at[t])
            pl.semaphore_wait(word.at[t], len(sides))
        tell(True, low.at[0])
        tell(False, high.at[0])

    @pl.loop(0, ne)
    def _(k):
        @pl.when(k != self_k)
        def _():
            plane_copy(k).start()

    with jax.named_scope("ready"):
        for distance in range(1, nr):
            @pl.when(r >= distance)
            def _():
                pl.semaphore_wait(low.at[distance - 1], 1)
                if distance + 1 < nr:
                    tell(True, low.at[distance])

            @pl.when(r + distance < nr)
            def _():
                pl.semaphore_wait(high.at[distance - 1], 1)
                if distance + 1 < nr:
                    tell(False, high.at[distance])

            if distance == 1:
                for k in pre:
                    send_cots(k, 1)

    send_targets(0, LEAD)

    with jax.named_scope("plane"):
        @pl.loop(0, ne)
        def _(k):
            @pl.when(k != self_k)
            def _():
                tok_wait(r, k)
                forward(r, k, True, tok.at[tok_at(r, k)])
                forward(r, k, False, tok.at[tok_at(r, k)])

    def relay_step(distance, k):
        for origin, up in ((r - distance, True), (r + distance, False)):
            @pl.when((origin >= 0) & (origin < nr))
            def _():
                tok_wait(origin, k)
                forward(origin, k, up, tok.at[tok_at(origin, k)])

    def own_column_last(k):
        k = jnp.where(e // nc == 0, (k + ne // 2 - 1) % (ne // 2), k)
        turned = jnp.where(k < ne // 4, k + ne // 4, ne // 2 - 1 - k)
        return jnp.where(core == 0, turned, k)

    sent = LEAD
    for distance in range(1, nr - 1):
        more = (C1, C2)[distance - 1] if distance < 3 else 0
        with jax.named_scope("relay%d" % distance):
            @pl.loop(0, ne)
            def _(k):
                relay_step(distance, k)

                if distance == 1:
                    @pl.when(k != self_k)
                    def _():
                        send_piece(k, r)

                if more:
                    @pl.when(k < more)
                    def _():
                        send_targets(sent + k, sent + k + 1)
        sent += more

    send_targets(sent, ne + lag)
    send_targets(0, ne // 2 + lag, send_last_block, ne // 2, own_column_last)

    planes = [jnp.where(r >= nr // 2, r + i, r + nr - i) % nr for i in range(nr)]

    with jax.named_scope("relay%d" % (nr - 1)):
        @pl.loop(0, ne)
        def _(k):
            relay_step(nr - 1, k)

    load_left.wait()
    tok_wait(r, self_k)
    step = tile_of(width, XM)
    for i, g in enumerate(planes):
        with jax.named_scope("x%d" % i):
            @pl.loop(0, width // step)
            def _(j):
                part = pl.ds(pl.multiple_of(j * step, step), step)
                columns = pl.ds(pl.multiple_of(g * group, group), group)
                tile = lax.dot_general(
                    left[part, :], tok[columns, :], (((1,), (1,)), ((), ())),
                    preferred_element_type=jnp.float32,
                ).astype(x.dtype)
                if i < nr - 2:
                    x[part, i * group:(i + 1) * group] = tile
                else:
                    at = (i - (nr - 2)) * half
                    x[part, (nr - 2) * group + at:(nr - 2) * group + at + half] = tile[:, :half]
                    x_late[part, at:at + half] = tile[:, half:]

    load_right.wait()

    def make_y(begin, blocks_of):
        for b in blocks_of:
            inside = slice(b * order, (b + 1) * order)
            y[begin:begin + group, inside] = jnp.dot(
                cot[begin:begin + group, inside], right[b], preferred_element_type=jnp.float32
            ).astype(y.dtype)

    early = (nr - 1) * group
    for i in range(nr - 2):
        with jax.named_scope("yw%d" % i):
            for sem in range(3):
                cot_wait(planes[i], sem)
        make_y(i * group, range(blocks))

    with jax.named_scope("ywhalf"):
        cot_wait(planes[nr - 2], 0)
        cot_wait(planes[nr - 1], 0)
    make_y(early - group, range(blocks))

    with jax.named_scope("P"):
        step = tile_of(order, PN)

        @pl.loop(0, order // step)
        def _(j):
            at = pl.multiple_of(j * step, step)
            part_ref[:, pl.ds(at, step)] = jnp.dot(
                x[...], y[:early, pl.ds(first + at, step)], preferred_element_type=jnp.float32
            )

    def send_wait(sem, data):
        pltpu.make_async_remote_copy(
            data, data, sem, tok_recv.at[0], device_id={"expert": e, "replica": (r + 1) % nr}
        ).wait_send()

    if first:
        with jax.named_scope("ywfirst"):
            cot_wait(planes[nr - 2], 1)
            cot_wait(planes[nr - 1], 1)
        make_y(early, range(blocks - 1))

        with jax.named_scope("done"):
            @pl.loop(0, first // step)
            def _(j):
                at = pl.ds(pl.multiple_of(j * step, step), step)
                done[:, at] = (
                    jnp.dot(x[...], y[:early, at], preferred_element_type=jnp.float32)
                    + jnp.dot(x_late[...], y[early:, at], preferred_element_type=jnp.float32)
                ).astype(done.dtype)

    with jax.named_scope("sends"):
        send_wait(plane_send, tok.at[pl.ds(0, group - rows)])
        send_wait(cot_send, cot.at[pl.ds(0, group * nr - rows)])
        for q in range(1, nr):
            @pl.when(r + 1 == q)
            def _():
                send_wait(up_send, tok.at[pl.ds(0, q * group)])

            @pl.when(nr - r == q)
            def _():
                send_wait(down_send, tok.at[pl.ds(0, q * group)])

    with jax.named_scope("ywlate"):
        cot_wait(planes[nr - 2], 2)
        cot_wait(planes[nr - 1], 2)


def finish_kernel(x_ref, cot_ref, right_ref, done_ref, part_ref, out_ref, y, out, sem):
    width, group = x_ref.shape
    total, order = cot_ref.shape[0], right_ref.shape[1]
    blocks = right_ref.shape[0]
    first = (blocks - 1) * order
    inside = slice(first, first + order)
    step = tile_of(width, FM)
    stores = []

    def store(data, at, columns):
        stores.append(pltpu.make_async_copy(data, out_ref.at[at, columns], sem.at[len(stores)]))
        stores[-1].start()

    tiles = [slice(i * step, (i + 1) * step) for i in range(width // step)]
    if first:
        for at in tiles:
            store(done_ref.at[at], at, slice(0, first))
    y[...] = jnp.dot(
        cot_ref[total - group:, inside], right_ref[blocks - 1], preferred_element_type=jnp.float32
    ).astype(y.dtype)
    for at in tiles:
        out[at, :] = (
            part_ref[at, :] + jnp.dot(x_ref[at, :], y[...], preferred_element_type=jnp.float32)
        ).astype(out.dtype)
        store(out.at[at], at, inside)
    for copy in stores:
        copy.wait()


def body(tokens_in, cotangents, left_root, right_root):
    ne, nr = lax.axis_size("expert"), lax.axis_size("replica")
    assert left_root.shape[0] == 1
    width = tokens_in.shape[1]
    columns = cotangents.shape[1] // nr
    total = tokens_in.shape[0] * nr
    group = tokens_in.shape[0]
    blocks, order = right_root.shape[1], right_root.shape[2]
    anywhere = pl.BlockSpec(memory_space=pl.ANY)
    vmem = pl.BlockSpec(memory_space=pltpu.VMEM)
    dtype = jnp.bfloat16
    dma = pltpu.SemaphoreType.DMA
    regular = pltpu.SemaphoreType.REGULAR
    kept = pl.pallas_call(
        functools.partial(route_kernel, ne, nr),
        out_shape=[
            pltpu.VMEM((width, group), dtype),
            pltpu.VMEM((total, columns), dtype),
            pltpu.VMEM((blocks, order, order), dtype),
            pltpu.VMEM((width, max(columns - order, 128)), dtype),
            pltpu.VMEM((width, order), jnp.float32),
        ],
        in_specs=[anywhere] * 4,
        out_specs=[vmem] * 5,
        scratch_shapes=[
            pltpu.VMEM((total, width), dtype),
            pltpu.VMEM((width, width), dtype),
            pltpu.VMEM((width, total - group), dtype),
            pltpu.VMEM((total, columns), dtype),
            regular((rounds_of(ne),)), regular((nr - 1,)), regular((nr - 1,)),
            dma, dma, dma, dma, dma((ne * nr,)), dma((3 * nr,)), dma((2,)),
        ],
        compiler_params=pltpu.CompilerParams(
            collective_id=0, has_side_effects=True, vmem_limit_bytes=34 * 1024 * 1024
        ),
    )(tokens_in, cotangents, left_root[0], right_root[0])
    out = pl.pallas_call(
        finish_kernel,
        out_shape=jax.ShapeDtypeStruct((width, columns), dtype),
        in_specs=[vmem] * 5,
        out_specs=anywhere,
        scratch_shapes=[
            pltpu.VMEM((group, order), dtype), pltpu.VMEM((width, order), dtype),
            dma((2 * (width // tile_of(width, FM)),)),
        ],
        compiler_params=pltpu.CompilerParams(vmem_limit_bytes=16 * 1024 * 1024),
    )(*kept)
    return out[None]


def solution(mesh):
    in_specs = (
        P(("expert", "replica"), None),
        P(("expert", "replica"), None),
        P("expert", None, None),
        P("expert", "replica", None, None),
    )
    out_specs = P("expert", None, "replica")
    return jax.shard_map(body, mesh=mesh, in_specs=in_specs, out_specs=out_specs, check_vma=False)
```
